32 devices in a mesh: cfg: 2 (over y), seq: 8 (over z, core), tp: 2 (over x).
Axes of the slice: x: 2, y: 2, z: 4, core: 2. Of those that a mesh axis runs over, the one named last changes fastest.
Arguments:
- queries: bfloat16 [2, 3840, 5120], P('cfg', 'seq', 'tp'), may hold values from -5 to 5
- keys: bfloat16 [2, 3840, 5120], P('cfg', 'seq', 'tp'), may hold values from -5 to 5
- values: bfloat16 [2, 3840, 5120], P('cfg', 'seq', 'tp'), may hold values from -5 to 5
- text_keys: bfloat16 [2, 512, 5120], P('cfg', None, 'tp'), may hold values from -7.5 to 7.5
- text_values: bfloat16 [2, 512, 5120], P('cfg', None, 'tp'), may hold values from -5 to 5
- prompt_lengths: int32 [2], P('cfg'), may hold values from 64 to 512
- frame_counts: int32 [8], P('seq'), may hold values from 240 to 480
- out_weight: bfloat16 [5120, 5120], P('tp'), may hold values from -0.5 to 0.5
Outputs:
- velocity: bfloat16 [3840, 5120], P('seq', ('tp', 'cfg'))
The draws below stay inside these ranges and needn't reach their ends.
All inputs are finite; a program needn't handle non-finite values.
Results may differ from the reference program's by a relative error of at most 0.015.
Values may be sent and summed in bfloat16 or wider, within the bound.
A program may use at most 320 MiB of HBM per device.

```python
import jax
import jax.numpy as jnp
from jax import lax

HEADS = 40
HEAD_DIM = 128
D = 5120
TEXT = 512
FRAME_SLOTS = 480
FRAMES = 8
TOKENS = 3840


def query_key_pair(key):
    base = jax.random.fold_in(key, 7)
    shape = (2, TOKENS, D)
    query_draw = jnp.clip(1.5 * jax.random.normal(jax.random.fold_in(base, 1), shape, jnp.float32), -5.0, 5.0)
    key_draw = jnp.clip(jax.random.normal(jax.random.fold_in(base, 2), shape, jnp.float32), -5.0, 5.0)
    return (query_draw, key_draw)


def draw_queries(key, part):
    return query_key_pair(key)[0].astype(jnp.bfloat16)


def draw_keys(key, part):
    return query_key_pair(key)[1].astype(jnp.bfloat16)


def touch_ends(entries, key, least, top_value):
    longest = entries.shape.index(max(entries.shape))
    spots = []
    for shift in (0, 1):
        where = [jax.random.randint(jax.random.fold_in(key, axis), (), 0, length) for axis, length in enumerate(entries.shape)]
        where[longest] = (where[longest] + shift) % entries.shape[longest]
        spots.append(tuple(where))
    return entries.at[spots[0]].set(least).at[spots[1]].set(top_value)


def levels(rng, shape, shards, smallest, high):
    def one(position, blocks):
        draws = jax.random.uniform(jax.random.fold_in(jax.random.fold_in(rng, 6), position), (blocks,), jnp.float32, smallest / len(shards), high / len(shards))
        return jnp.repeat(jnp.exp(draws), shape[position] // blocks).reshape((-1,) + (1,) * (len(shape) - position - 1))

    gain = one(*shards[0])
    for cut in shards[1:]:
        gain = gain * one(*cut)
    return gain


def normal_values(stream_key, extent, scale, limit, shards=(), kind=jnp.bfloat16):
    level = levels(stream_key, extent, shards, -0.22, 0.18) if shards else 1.0
    array = jax.random.normal(stream_key, extent, jnp.float32) * scale * level
    return jnp.minimum(jnp.maximum(array, -limit), limit).astype(kind)


def setup_inputs(seed: int = 0) -> dict:
    seeds = jax.random.split(jax.random.key(seed), 9)
    return {
        "queries": draw_queries(jax.random.fold_in(seeds[8], 71), 0),
        "keys": draw_keys(jax.random.fold_in(seeds[8], 71), 0),
        "values": normal_values(seeds[2], (2, TOKENS, D), 1.0, 5.0, ((0, 2), (1, 8), (2, 2))),
        "text_keys": normal_values(seeds[3], (2, TEXT, D), 1.5, 7.5, ((0, 2), (2, 2))),
        "text_values": normal_values(seeds[4], (2, TEXT, D), 1.0, 5.0, ((0, 2), (2, 2))),
        "prompt_lengths": jax.random.randint(seeds[5], (2,), TEXT // 8, TEXT + 1).astype(jnp.int32),
        "frame_counts": touch_ends(jax.random.randint(seeds[6], (FRAMES,), FRAME_SLOTS // 2, FRAME_SLOTS + 1), jax.random.fold_in(seeds[6], 1), FRAME_SLOTS // 2, FRAME_SLOTS).astype(jnp.int32),
        "out_weight": normal_values(seeds[7], (D, D), (D // 32) ** -0.5, 0.5, ((0, 2),)),
    }


GUIDANCE = 5.0
RESCALE = 0.7
NEGATIVE = -1e+30

def video_valid(frame_counts):
    positions = jnp.arange(TOKENS, dtype=jnp.int32)
    return positions % FRAME_SLOTS < frame_counts[positions // FRAME_SLOTS]

def branch_output(query_rows, key_rows, value_rows, text_key_rows, text_value_rows, length, video_mask, out_weight):
    text_mask = jnp.arange(TEXT, dtype=jnp.int32) < length
    full_mask = jnp.concatenate([text_mask, video_mask])
    all_keys = jnp.concatenate([text_key_rows, key_rows], axis=0)
    all_values = jnp.concatenate([text_value_rows, value_rows], axis=0)
    key_total = all_keys.shape[0]
    query_heads = jnp.transpose(query_rows.reshape(TOKENS, HEADS, HEAD_DIM), (1, 0, 2))
    key_heads = jnp.transpose(all_keys.reshape(key_total, HEADS, HEAD_DIM), (1, 0, 2))
    value_heads = jnp.transpose(all_values.reshape(key_total, HEADS, HEAD_DIM), (1, 0, 2))

    def one_head(operands):
        query_head, key_head, value_head = operands
        scores = jnp.dot(query_head, key_head.T, preferred_element_type=jnp.float32) * HEAD_DIM ** (-0.5)
        scores = jnp.where(full_mask[None, :], scores, NEGATIVE)
        row_max = lax.optimization_barrier(jnp.max(scores, axis=1, keepdims=True))
        weights = jnp.exp(scores - row_max)
        weight_sum = lax.optimization_barrier(jnp.sum(weights, axis=1, keepdims=True))
        mixed_rows = jnp.dot(weights.astype(jnp.bfloat16), value_head, preferred_element_type=jnp.float32)
        return (mixed_rows / weight_sum).astype(jnp.bfloat16)
    heads_out = lax.map(one_head, (query_heads, key_heads, value_heads))
    attended = jnp.transpose(heads_out, (1, 0, 2)).reshape(TOKENS, HEADS * HEAD_DIM)
    return jnp.dot(attended, out_weight, preferred_element_type=jnp.float32).astype(jnp.bfloat16)

def reference(queries, keys, values, text_keys, text_values, prompt_lengths, frame_counts, out_weight):
    video_mask = video_valid(frame_counts)
    conditional = branch_output(queries[0], keys[0], values[0], text_keys[0], text_values[0], prompt_lengths[0], video_mask, out_weight).astype(jnp.float32)
    unconditional = branch_output(queries[1], keys[1], values[1], text_keys[1], text_values[1], prompt_lengths[1], video_mask, out_weight).astype(jnp.float32)
    guided = unconditional + GUIDANCE * (conditional - unconditional)
    token_weights = video_mask.astype(jnp.float32)
    valid_total = jnp.sum(frame_counts).astype(jnp.float32)

    def moment(field_rows):
        return jnp.dot(token_weights, field_rows, precision=lax.Precision.HIGHEST) / valid_total
    guided_mean = moment(guided)
    guided_var = moment(guided * guided) - guided_mean * guided_mean
    cond_mean = moment(conditional)
    cond_var = moment(conditional * conditional) - cond_mean * cond_mean
    std_ratio = jnp.sqrt((cond_var + 1.0) / (guided_var + 1.0))
    factor = RESCALE * std_ratio + (1.0 - RESCALE)
    return (guided_mean + (guided - guided_mean) * factor).astype(jnp.bfloat16)
```

```python
import functools

import jax
import jax.numpy as jnp
from jax import lax
from jax.experimental import pallas as pl
from jax.experimental.pallas import tpu as pltpu
from jax.sharding import PartitionSpec as P

HEAD_DIM = 128
GUIDANCE = 5.0
RESCALE = 0.7
NEGATIVE = -1e30
LOG2E = 1.4426950408889634
CORES = 2
MESH = pl.DeviceIdType.MESH


def chunk_rows(total, limit):
    for unit in (256, 128, 16):
        for size in range(limit // unit * unit, 0, -unit):
            if total % size == 0:
                return size
    return total


def attention_kernel(
    n, chips, group, rows, text,
    q, k, v, tk, tv, counts, lengths,
    out,
    qb, kb, vb, tkb, tvb, cb, bias, tbias, ob,
    send, recv, fsend, frecv, csend, crecv, local, tlocal, osend, orecv,
):
    me = lax.axis_index("seq")
    core = lax.rem(me, CORES)
    chip = lax.div(me, CORES)
    partner = chip * CORES + (CORES - 1 - core)
    scale = LOG2E * HEAD_DIM ** (-0.5)

    def cols(owner, head):
        return pl.ds(pl.multiple_of((owner * group + head) * HEAD_DIM, HEAD_DIM), HEAD_DIM)

    def slot(index):
        return pl.ds(pl.multiple_of(index * rows, 16), rows)

    def chip_at(step):
        return lax.rem(chip + step, chips)

    def chip_back(step):
        return lax.rem(chip + chips - step, chips)

    barrier = pltpu.get_barrier_semaphore()
    for step in range(1, n):
        pl.semaphore_signal(
            barrier, inc=1, device_id={"seq": lax.rem(me + step, n)}, device_id_type=MESH
        )
    pl.semaphore_wait(barrier, n - 1)

    def count_copy(step):
        return pltpu.make_async_remote_copy(
            src_ref=counts, dst_ref=cb.at[me], send_sem=csend.at[step - 1],
            recv_sem=crecv.at[step - 1],
            device_id={"seq": lax.rem(me + step, n)}, device_id_type=MESH,
        )

    def block_copies(head, step):
        target = chip_at(step)
        device = {"seq": target * CORES + core}
        made = []
        for index, (src, dst) in enumerate(
            ((k, kb.at[head, slot(me)]), (v, vb.at[head, slot(me)]), (q, qb.at[head, chip]))
        ):
            made.append(pltpu.make_async_remote_copy(
                src_ref=src.at[:, cols(target, head)], dst_ref=dst,
                send_sem=send.at[index, head, step - 1],
                recv_sem=recv.at[index, head, step - 1],
                device_id=device, device_id_type=MESH,
            ))
        return made

    def own_copies(head):
        return [
            pltpu.make_async_copy(k.at[:, cols(chip, head)], kb.at[head, slot(me)], local.at[0, head]),
            pltpu.make_async_copy(v.at[:, cols(chip, head)], vb.at[head, slot(me)], local.at[1, head]),
            pltpu.make_async_copy(q.at[:, cols(chip, head)], qb.at[head, chip], local.at[2, head]),
            pltpu.make_async_copy(tk.at[:, cols(chip, head)], tkb.at[head], tlocal.at[0, head]),
            pltpu.make_async_copy(tv.at[:, cols(chip, head)], tvb.at[head], tlocal.at[1, head]),
        ]

    def own_forward(head):
        return [
            pltpu.make_async_remote_copy(
                src_ref=src.at[:, cols(chip, head)], dst_ref=dst.at[head, slot(me)],
                send_sem=fsend.at[index, head, 0], recv_sem=frecv.at[index, head, 0],
                device_id={"seq": partner}, device_id_type=MESH,
            )
            for index, (src, dst) in enumerate(((k, kb), (v, vb)))
        ]

    def forward(index, head, step):
        buf = (kb, vb)[index]
        where = slot(chip_back(step) * CORES + core)
        return pltpu.make_async_remote_copy(
            src_ref=buf.at[head, where], dst_ref=buf.at[head, where],
            send_sem=fsend.at[index, head, step], recv_sem=frecv.at[index, head, step],
            device_id={"seq": partner}, device_id_type=MESH,
        )

    def out_copy(head, step):
        target = chip_at(step)
        return pltpu.make_async_remote_copy(
            src_ref=ob.at[head, target], dst_ref=out.at[:, cols(chip, head)],
            send_sem=osend.at[head, step], recv_sem=orecv.at[head, step],
            device_id={"seq": target * CORES + core}, device_id_type=MESH,
        )

    def own_out(head):
        return pltpu.make_async_copy(
            ob.at[head, chip], out.at[:, cols(chip, head)], osend.at[head, 0]
        )

    for step in range(1, n):
        count_copy(step).start()

    def start_head(head, _):
        for step in range(1, chips):
            for copy in block_copies(head, step):
                copy.start()
        for copy in own_copies(head):
            copy.start()
        for copy in own_forward(head):
            copy.start()
        return 0

    lax.fori_loop(0, group, start_head, 0)

    cb[me] = counts[...]
    for step in range(1, n):
        count_copy(step).wait()
    lane = lax.broadcasted_iota(jnp.int32, (rows, HEAD_DIM), 1)
    place = lax.broadcasted_iota(jnp.int32, (rows, HEAD_DIM), 0)
    for source in range(n):
        limit = cb[source][0:1, :]
        bias[source * rows:(source + 1) * rows, :] = jnp.where(
            (lane == 0) & (place >= limit), NEGATIVE, 0.0
        ).astype(jnp.bfloat16)
    tlane = lax.broadcasted_iota(jnp.int32, (text, HEAD_DIM), 1)
    tplace = lax.broadcasted_iota(jnp.int32, (text, HEAD_DIM), 0)
    tbias[...] = jnp.where(
        (tlane == 0) & (tplace >= lengths[0:1, :]), NEGATIVE, 0.0
    ).astype(jnp.bfloat16)

    total = n * rows
    size = chunk_rows(total, 768)

    def ones(length):
        return jnp.where(
            lax.broadcasted_iota(jnp.int32, (length, HEAD_DIM), 1) == 0, 1.0, 0.0
        ).astype(jnp.bfloat16)

    def one_head(head, _):
        for copy in own_copies(head):
            copy.wait()
        for step in range(1, chips):
            made = block_copies(head, step)
            for index in range(2):
                made[index].wait()
                forward(index, head, step).start()
            made[2].wait()
        for copy in own_forward(head):
            copy.wait()
        for step in range(1, chips):
            for index in range(2):
                forward(index, head, step).wait()

        def one_block(step):
            target = chip_at(step)
            query = jnp.concatenate([qb[head, target], ones(rows)], axis=1)

            def piece(state, keys, masks, vals):
                keys = jnp.concatenate([keys, masks], axis=1)
                vals = jnp.concatenate([vals, ones(vals.shape[0])], axis=1)
                scores = lax.dot_general(
                    query, keys, (((1,), (1,)), ((), ())), preferred_element_type=jnp.float32
                )
                high = jnp.max(scores, axis=1, keepdims=True) * scale
                if state is not None:
                    high = jnp.maximum(high, state[0])
                weights = jnp.exp2(scores * scale - high).astype(jnp.bfloat16)
                mixed = jnp.dot(weights, vals, preferred_element_type=jnp.float32)
                if state is not None:
                    mixed = mixed + state[1] * jnp.exp2(state[0] - high)
                return (high, mixed)

            state = piece(None, tkb[head], tbias[...], tvb[head])
            for start in range(0, total, size):
                span = pl.ds(start, size)
                state = piece(state, kb[head, span], bias[span, :], vb[head, span])
            mixed = state[1]
            ob[head, target] = (
                mixed[:, :HEAD_DIM] / mixed[:, HEAD_DIM:HEAD_DIM + 1]
            ).astype(jnp.bfloat16)

        def far_block(step, _):
            one_block(step)
            out_copy(head, step).start()
            return 0

        lax.fori_loop(1, chips, far_block, 0)
        one_block(0)
        own_out(head).start()
        return 0

    lax.fori_loop(0, group, one_head, 0)

    def finish(head, _):
        for step in range(1, chips):
            out_copy(head, step).wait()
        own_out(head).wait()
        return 0

    lax.fori_loop(0, group, finish, 0)


def attention(queries, keys, values, text_keys, text_values, prompt_lengths, frame_counts, n):
    rows, width = queries.shape
    text = text_keys.shape[0]
    chips = n // CORES
    heads = width // HEAD_DIM
    group = heads // chips
    counts = jnp.broadcast_to(frame_counts.reshape(1, 1), (8, HEAD_DIM))
    lengths = jnp.broadcast_to(prompt_lengths.reshape(1, 1), (8, HEAD_DIM))
    bf16 = jnp.bfloat16
    total = n * rows
    hbm = pl.BlockSpec(memory_space=pl.ANY)
    vmem = pl.BlockSpec(memory_space=pltpu.VMEM)
    dma = pltpu.SemaphoreType.DMA
    return pl.pallas_call(
        functools.partial(attention_kernel, n, chips, group, rows, text),
        out_shape=jax.ShapeDtypeStruct((rows, width), bf16),
        in_specs=[hbm] * 5 + [vmem] * 2,
        out_specs=hbm,
        scratch_shapes=[
            pltpu.VMEM((group, chips, rows, HEAD_DIM), bf16),
            pltpu.VMEM((group, total, HEAD_DIM), bf16),
            pltpu.VMEM((group, total, HEAD_DIM), bf16),
            pltpu.VMEM((group, text, HEAD_DIM), bf16),
            pltpu.VMEM((group, text, HEAD_DIM), bf16),
            pltpu.VMEM((n, 8, HEAD_DIM), jnp.int32),
            pltpu.VMEM((total, HEAD_DIM), bf16),
            pltpu.VMEM((text, HEAD_DIM), bf16),
            pltpu.VMEM((group, chips, rows, HEAD_DIM), bf16),
            dma((3, group, chips - 1)),
            dma((3, group, chips - 1)),
            dma((2, group, chips)),
            dma((2, group, chips)),
            dma((n - 1,)),
            dma((n - 1,)),
            dma((3, group)),
            dma((2, group)),
            dma((group, chips)),
            dma((group, chips)),
        ],
        compiler_params=pltpu.CompilerParams(
            collective_id=0, has_side_effects=True, vmem_limit_bytes=62 * 1024 * 1024
        ),
    )(queries, keys, values, text_keys, text_values, counts, lengths)


def frame_valid(positions, counts_table, slots):
    frame_index = positions // slots
    slot_index = positions % slots
    frame_ids = jnp.arange(counts_table.shape[0], dtype=jnp.int32)
    frame_limit = jnp.sum(
        jnp.where(frame_index[:, None] == frame_ids[None, :], counts_table[None, :], 0), axis=1
    )
    return slot_index < frame_limit


def attend_block(carry, key_rows, value_rows, query_heads, key_mask):
    row_max, weight_sum, mixed_sum = carry
    head_count = query_heads.shape[1]
    key_heads = key_rows.reshape(key_rows.shape[0], head_count, HEAD_DIM)
    value_heads = value_rows.reshape(value_rows.shape[0], head_count, HEAD_DIM)
    scores = jnp.einsum(
        "qhd,khd->hqk", query_heads, key_heads, preferred_element_type=jnp.float32
    ) * HEAD_DIM ** (-0.5)
    scores = jnp.where(key_mask[None, None, :], scores, NEGATIVE)
    new_max = jnp.maximum(row_max, jnp.max(scores, axis=2))
    shrink = jnp.exp(row_max - new_max)
    weights = jnp.exp(scores - new_max[:, :, None])
    weight_sum = weight_sum * shrink + jnp.sum(weights, axis=2)
    mixed_sum = mixed_sum * shrink[:, :, None] + jnp.einsum(
        "hqk,khd->hqd",
        weights.astype(jnp.bfloat16),
        value_heads,
        preferred_element_type=jnp.float32,
    )
    return (new_max, weight_sum, mixed_sum)


def gathered_attention(
    queries, keys, values, text_keys, text_values, prompt_lengths, frame_counts, n
):
    row_count, head_cols = queries.shape
    head_count = head_cols // HEAD_DIM
    all_counts = lax.all_gather(frame_counts, "seq", axis=0, tiled=True)
    query_heads = queries.reshape(row_count, head_count, HEAD_DIM)
    text_mask = jnp.arange(text_keys.shape[0], dtype=jnp.int32) < prompt_lengths[0]
    empty_state = (
        jnp.full((head_count, row_count), NEGATIVE, jnp.float32),
        jnp.zeros((head_count, row_count), jnp.float32),
        jnp.zeros((head_count, row_count, HEAD_DIM), jnp.float32),
    )
    text_state = attend_block(empty_state, text_keys, text_values, query_heads, text_mask)
    key_rows = lax.all_gather(keys, "seq", axis=0, tiled=True)
    value_rows = lax.all_gather(values, "seq", axis=0, tiled=True)
    positions = jnp.arange(key_rows.shape[0], dtype=jnp.int32)
    _, weight_sum, mixed_sum = attend_block(
        text_state, key_rows, value_rows, query_heads,
        frame_valid(positions, all_counts, row_count // frame_counts.shape[0]),
    )
    return (
        jnp.transpose(mixed_sum / weight_sum[:, :, None], (1, 0, 2))
        .reshape(row_count, head_cols)
        .astype(jnp.bfloat16)
    )


def body(n, cfgs, queries, keys, values, text_keys, text_values, prompt_lengths, frame_counts, out_weight):
    rows, head_cols = queries.shape[1:]
    split = n % CORES == 0 and (head_cols // HEAD_DIM) % (n // CORES) == 0
    attend = attention if split and frame_counts.shape[0] == 1 else gathered_attention
    attended = attend(
        queries[0], keys[0], values[0], text_keys[0], text_values[0],
        prompt_lengths, frame_counts, n,
    )
    branch = lax.psum_scatter(
        lax.dot_general(
            out_weight, attended, (((0,), (1,)), ((), ())), preferred_element_type=jnp.float32
        ).astype(jnp.bfloat16),
        "tp",
        scatter_dimension=0,
        tiled=True,
    )
    half = branch.shape[0] // cfgs
    mine = lax.axis_index("cfg")
    kept = lax.dynamic_slice_in_dim(branch, mine * half, half, 0)
    given = lax.dynamic_slice_in_dim(branch, (1 - mine) * half, half, 0)
    other = lax.ppermute(given, "cfg", [(0, 1), (1, 0)])
    first = mine == 0
    conditional = jnp.where(first, kept, other).astype(jnp.float32)
    unconditional = jnp.where(first, other, kept).astype(jnp.float32)
    guided = unconditional + GUIDANCE * (conditional - unconditional)
    valid = (jnp.arange(rows, dtype=jnp.int32) < frame_counts[0])[None, :]

    def local_sum(field):
        return jnp.sum(jnp.where(valid, field, 0.0), axis=1)

    sums = lax.psum(
        jnp.stack([
            local_sum(guided),
            local_sum(guided * guided),
            local_sum(conditional),
            local_sum(conditional * conditional),
            jnp.full((half,), frame_counts[0].astype(jnp.float32)),
        ]),
        "seq",
    )
    means = sums[:4] / sums[4:5]
    guided_mean = means[0]
    guided_var = means[1] - guided_mean * guided_mean
    cond_var = means[3] - means[2] * means[2]
    std_ratio = jnp.sqrt((cond_var + 1.0) / (guided_var + 1.0))
    factor = RESCALE * std_ratio + (1.0 - RESCALE)
    velocity = guided_mean[:, None] + (guided - guided_mean[:, None]) * factor[:, None]
    return velocity.astype(jnp.bfloat16).T


def solution(mesh):
    placed = (
        P("cfg", "seq", "tp"),
        P("cfg", "seq", "tp"),
        P("cfg", "seq", "tp"),
        P("cfg", None, "tp"),
        P("cfg", None, "tp"),
        P("cfg"),
        P("seq"),
        P("tp", None),
    )
    return jax.shard_map(
        functools.partial(body, mesh.shape["seq"], mesh.shape["cfg"]),
        mesh=mesh, in_specs=placed, out_specs=P("seq", ("tp", "cfg")), check_vma=False,
    )
```

```python
import functools

import jax
import jax.numpy as jnp
from jax import lax
from jax.experimental import pallas as pl
from jax.experimental.pallas import tpu as pltpu
from jax.sharding import PartitionSpec as P

HEAD_DIM = 128
GUIDANCE = 5.0
RESCALE = 0.7
NEGATIVE = -1e30
LOG2E = 1.4426950408889634
CORES = 2
MESH = pl.DeviceIdType.MESH


def chunk_rows(total, limit):
    for unit in (256, 128, 16):
        for size in range(limit // unit * unit, 0, -unit):
            if total % size == 0:
                return size
    return total


def attention_kernel(
    n, chips, group, rows, text,
    q, k, v, tk, tv, counts, lengths,
    out,
    qb, kb, vb, tkb, tvb, cb, bias, tbias, ob,
    send, recv, fsend, frecv, csend, crecv, local, tlocal, osend, orecv,
):
    me = lax.axis_index("seq")
    core = lax.rem(me, CORES)
    chip = lax.div(me, CORES)
    partner = chip * CORES + (CORES - 1 - core)
    scale = LOG2E * HEAD_DIM ** (-0.5)

    def cols(owner, head):
        return pl.ds(pl.multiple_of((owner * group + head) * HEAD_DIM, HEAD_DIM), HEAD_DIM)

    def slot(index):
        return pl.ds(pl.multiple_of(index * rows, 16), rows)

    def chip_at(step):
        return lax.rem(chip + step, chips)

    def chip_back(step):
        return lax.rem(chip + chips - step, chips)

    barrier = pltpu.get_barrier_semaphore()
    for step in range(1, n):
        pl.semaphore_signal(
            barrier, inc=1, device_id={"seq": lax.rem(me + step, n)}, device_id_type=MESH
        )
    pl.semaphore_wait(barrier, n - 1)

    def count_copy(step):
        return pltpu.make_async_remote_copy(
            src_ref=counts, dst_ref=cb.at[me], send_sem=csend.at[step - 1],
            recv_sem=crecv.at[step - 1],
            device_id={"seq": lax.rem(me + step, n)}, device_id_type=MESH,
        )

    def block_copies(head, step):
        target = chip_at(step)
        device = {"seq": target * CORES + core}
        made = []
        for index, (src, dst) in enumerate(
            ((k, kb.at[head, slot(me)]), (v, vb.at[head, slot(me)]), (q, qb.at[head, chip]))
        ):
            made.append(pltpu.make_async_remote_copy(
                src_ref=src.at[:, cols(target, head)], dst_ref=dst,
                send_sem=send.at[index, head, step - 1],
                recv_sem=recv.at[index, head, step - 1],
                device_id=device, device_id_type=MESH,
            ))
        return made

    def own_copies(head):
        return [
            pltpu.make_async_copy(k.at[:, cols(chip, head)], kb.at[head, slot(me)], local.at[0, head]),
            pltpu.make_async_copy(v.at[:, cols(chip, head)], vb.at[head, slot(me)], local.at[1, head]),
            pltpu.make_async_copy(q.at[:, cols(chip, head)], qb.at[head, chip], local.at[2, head]),
            pltpu.make_async_copy(tk.at[:, cols(chip, head)], tkb.at[head], tlocal.at[0, head]),
            pltpu.make_async_copy(tv.at[:, cols(chip, head)], tvb.at[head], tlocal.at[1, head]),
        ]

    def own_forward(head):
        return [
            pltpu.make_async_remote_copy(
                src_ref=src.at[:, cols(chip, head)], dst_ref=dst.at[head, slot(me)],
                send_sem=fsend.at[index, head, 0], recv_sem=frecv.at[index, head, 0],
                device_id={"seq": partner}, device_id_type=MESH,
            )
            for index, (src, dst) in enumerate(((k, kb), (v, vb)))
        ]

    def forward(index, head, step):
        buf = (kb, vb)[index]
        where = slot(chip_back(step) * CORES + core)
        return pltpu.make_async_remote_copy(
            src_ref=buf.at[head, where], dst_ref=buf.at[head, where],
            send_sem=fsend.at[index, head, step], recv_sem=frecv.at[index, head, step],
            device_id={"seq": partner}, device_id_type=MESH,
        )

    def out_copy(head, step):
        target = chip_at(step)
        return pltpu.make_async_remote_copy(
            src_ref=ob.at[head, target], dst_ref=out.at[:, cols(chip, head)],
            send_sem=osend.at[head, step], recv_sem=orecv.at[head, step],
            device_id={"seq": target * CORES + core}, device_id_type=MESH,
        )

    def own_out(head):
        return pltpu.make_async_copy(
            ob.at[head, chip], out.at[:, cols(chip, head)], osend.at[head, 0]
        )

    for step in range(1, n):
        count_copy(step).start()

    def start_head(head, _):
        for step in range(1, chips):
            for copy in block_copies(head, step):
                copy.start()
        for copy in own_copies(head):
            copy.start()
        for copy in own_forward(head):
            copy.start()
        return 0

    lax.fori_loop(0, group, start_head, 0)

    cb[me] = counts[...]
    for step in range(1, n):
        count_copy(step).wait()
    lane = lax.broadcasted_iota(jnp.int32, (rows, HEAD_DIM), 1)
    place = lax.broadcasted_iota(jnp.int32, (rows, HEAD_DIM), 0)
    for source in range(n):
        limit = cb[source][0:1, :]
        bias[source * rows:(source + 1) * rows, :] = jnp.where(
            (lane == 0) & (place >= limit), NEGATIVE, 0.0
        ).astype(jnp.bfloat16)
    tlane = lax.broadcasted_iota(jnp.int32, (text, HEAD_DIM), 1)
    tplace = lax.broadcasted_iota(jnp.int32, (text, HEAD_DIM), 0)
    tbias[...] = jnp.where(
        (tlane == 0) & (tplace >= lengths[0:1, :]), NEGATIVE, 0.0
    ).astype(jnp.bfloat16)

    total = n * rows
    size = chunk_rows(total, 768)

    def ones(length):
        return jnp.where(
            lax.broadcasted_iota(jnp.int32, (length, HEAD_DIM), 1) == 0, 1.0, 0.0
        ).astype(jnp.bfloat16)

    def one_head(head, _):
        for copy in own_copies(head):
            copy.wait()
        for step in range(1, chips):
            made = block_copies(head, step)
            for index in range(2):
                made[index].wait()
                forward(index, head, step).start()
            made[2].wait()
        for copy in own_forward(head):
            copy.wait()
        for step in range(1, chips):
            for index in range(2):
                forward(index, head, step).wait()

        def one_block(step):
            target = chip_at(step)
            query = jnp.concatenate([qb[head, target], ones(rows)], axis=1)

            def piece(state, keys, masks, vals):
                keys = jnp.concatenate([keys, masks], axis=1)
                vals = jnp.concatenate([vals, ones(vals.shape[0])], axis=1)
                scores = lax.dot_general(
                    query, keys, (((1,), (1,)), ((), ())), preferred_element_type=jnp.float32
                )
                high = jnp.max(scores, axis=1, keepdims=True) * scale
                if state is not None:
                    high = jnp.maximum(high, state[0])
                weights = jnp.exp2(scores * scale - high).astype(jnp.bfloat16)
                mixed = jnp.dot(weights, vals, preferred_element_type=jnp.float32)
                if state is not None:
                    mixed = mixed + state[1] * jnp.exp2(state[0] - high)
                return (high, mixed)

            state = piece(None, tkb[head], tbias[...], tvb[head])
            for start in range(0, total, size):
                span = pl.ds(start, size)
                state = piece(state, kb[head, span], bias[span, :], vb[head, span])
            mixed = state[1]
            ob[head, target] = (
                mixed[:, :HEAD_DIM] / mixed[:, HEAD_DIM:HEAD_DIM + 1]
            ).astype(jnp.bfloat16)

        def far_block(step, _):
            one_block(step)
            out_copy(head, step).start()
            return 0

        lax.fori_loop(1, chips, far_block, 0)
        one_block(0)
        own_out(head).start()
        return 0

    lax.fori_loop(0, group, one_head, 0)

    def finish(head, _):
        for step in range(1, chips):
            out_copy(head, step).wait()
        own_out(head).wait()
        return 0

    lax.fori_loop(0, group, finish, 0)


def attention(queries, keys, values, text_keys, text_values, prompt_lengths, frame_counts, n):
    rows, width = queries.shape
    text = text_keys.shape[0]
    chips = n // CORES
    heads = width // HEAD_DIM
    group = heads // chips
    counts = jnp.broadcast_to(frame_counts.reshape(1, 1), (8, HEAD_DIM))
    lengths = jnp.broadcast_to(prompt_lengths.reshape(1, 1), (8, HEAD_DIM))
    bf16 = jnp.bfloat16
    total = n * rows
    hbm = pl.BlockSpec(memory_space=pl.ANY)
    vmem = pl.BlockSpec(memory_space=pltpu.VMEM)
    dma = pltpu.SemaphoreType.DMA
    return pl.pallas_call(
        functools.partial(attention_kernel, n, chips, group, rows, text),
        out_shape=jax.ShapeDtypeStruct((rows, width), bf16),
        in_specs=[hbm] * 5 + [vmem] * 2,
        out_specs=hbm,
        scratch_shapes=[
            pltpu.VMEM((group, chips, rows, HEAD_DIM), bf16),
            pltpu.VMEM((group, total, HEAD_DIM), bf16),
            pltpu.VMEM((group, total, HEAD_DIM), bf16),
            pltpu.VMEM((group, text, HEAD_DIM), bf16),
            pltpu.VMEM((group, text, HEAD_DIM), bf16),
            pltpu.VMEM((n, 8, HEAD_DIM), jnp.int32),
            pltpu.VMEM((total, HEAD_DIM), bf16),
            pltpu.VMEM((text, HEAD_DIM), bf16),
            pltpu.VMEM((group, chips, rows, HEAD_DIM), bf16),
            dma((3, group, chips - 1)),
            dma((3, group, chips - 1)),
            dma((2, group, chips)),
            dma((2, group, chips)),
            dma((n - 1,)),
            dma((n - 1,)),
            dma((3, group)),
            dma((2, group)),
            dma((group, chips)),
            dma((group, chips)),
        ],
        compiler_params=pltpu.CompilerParams(
            collective_id=0, has_side_effects=True, vmem_limit_bytes=62 * 1024 * 1024
        ),
    )(queries, keys, values, text_keys, text_values, counts, lengths)


def frame_valid(positions, counts_table, slots):
    frame_index = positions // slots
    slot_index = positions % slots
    frame_ids = jnp.arange(counts_table.shape[0], dtype=jnp.int32)
    frame_limit = jnp.sum(
        jnp.where(frame_index[:, None] == frame_ids[None, :], counts_table[None, :], 0), axis=1
    )
    return slot_index < frame_limit


def attend_block(carry, key_rows, value_rows, query_heads, key_mask):
    row_max, weight_sum, mixed_sum = carry
    head_count = query_heads.shape[1]
    key_heads = key_rows.reshape(key_rows.shape[0], head_count, HEAD_DIM)
    value_heads = value_rows.reshape(value_rows.shape[0], head_count, HEAD_DIM)
    scores = jnp.einsum(
        "qhd,khd->hqk", query_heads, key_heads, preferred_element_type=jnp.float32
    ) * HEAD_DIM ** (-0.5)
    scores = jnp.where(key_mask[None, None, :], scores, NEGATIVE)
    new_max = jnp.maximum(row_max, jnp.max(scores, axis=2))
    shrink = jnp.exp(row_max - new_max)
    weights = jnp.exp(scores - new_max[:, :, None])
    weight_sum = weight_sum * shrink + jnp.sum(weights, axis=2)
    mixed_sum = mixed_sum * shrink[:, :, None] + jnp.einsum(
        "hqk,khd->hqd",
        weights.astype(jnp.bfloat16),
        value_heads,
        preferred_element_type=jnp.float32,
    )
    return (new_max, weight_sum, mixed_sum)


def gathered_attention(
    queries, keys, values, text_keys, text_values, prompt_lengths, frame_counts, n
):
    row_count, head_cols = queries.shape
    head_count = head_cols // HEAD_DIM
    all_counts = lax.all_gather(frame_counts, "seq", axis=0, tiled=True)
    query_heads = queries.reshape(row_count, head_count, HEAD_DIM)
    text_mask = jnp.arange(text_keys.shape[0], dtype=jnp.int32) < prompt_lengths[0]
    empty_state = (
        jnp.full((head_count, row_count), NEGATIVE, jnp.float32),
        jnp.zeros((head_count, row_count), jnp.float32),
        jnp.zeros((head_count, row_count, HEAD_DIM), jnp.float32),
    )
    text_state = attend_block(empty_state, text_keys, text_values, query_heads, text_mask)
    key_rows = lax.all_gather(keys, "seq", axis=0, tiled=True)
    value_rows = lax.all_gather(values, "seq", axis=0, tiled=True)
    positions = jnp.arange(key_rows.shape[0], dtype=jnp.int32)
    _, weight_sum, mixed_sum = attend_block(
        text_state, key_rows, value_rows, query_heads,
        frame_valid(positions, all_counts, row_count // frame_counts.shape[0]),
    )
    return (
        jnp.transpose(mixed_sum / weight_sum[:, :, None], (1, 0, 2))
        .reshape(row_count, head_cols)
        .astype(jnp.bfloat16)
    )


PIECES = 2


def tail_kernel(
    n, rows, part,
    att, w, counts,
    out,
    ab, wb, sb, rb, own, yb, yr, gb, st, sg,
    asem, wsem, xsend, xrecv, ysend, yrecv, ssend, srecv,
):
    me = lax.axis_index("seq")
    t = lax.axis_index("tp")
    c = lax.axis_index("cfg")
    steps = 2 * PIECES
    width = PIECES * part

    def column(side, index):
        far = lax.div(index, PIECES)
        branch = far * c + (1 - far) * (1 - c)
        return (side * 2 + branch) * width + lax.rem(index, PIECES) * part

    def weight_copy(j):
        far = lax.div(j, steps)
        side = far * t + (1 - far) * (1 - t)
        start = pl.multiple_of(column(side, lax.rem(j, steps)), HEAD_DIM)
        return pltpu.make_async_copy(w.at[:, pl.ds(start, part)], wb.at[j], wsem.at[j])

    load = pltpu.make_async_copy(att, ab, asem)
    load.start()

    def start_weight(j, _):
        weight_copy(j).start()
        return 0

    lax.fori_loop(0, 2 * steps, start_weight, 0)

    barrier = pltpu.get_barrier_semaphore()
    pl.semaphore_signal(barrier, inc=1, device_id={"tp": 1 - t}, device_id_type=MESH)
    pl.semaphore_signal(barrier, inc=1, device_id={"cfg": 1 - c}, device_id_type=MESH)
    for step in range(1, n):
        pl.semaphore_signal(
            barrier, inc=1, device_id={"seq": lax.rem(me + step, n)}, device_id_type=MESH
        )
    pl.semaphore_wait(barrier, n + 1)

    def x_copy(i):
        return pltpu.make_async_remote_copy(
            src_ref=sb.at[i], dst_ref=rb.at[i], send_sem=xsend.at[i], recv_sem=xrecv.at[i],
            device_id={"tp": 1 - t}, device_id_type=MESH,
        )

    def y_copy(i):
        return pltpu.make_async_remote_copy(
            src_ref=yb.at[i], dst_ref=yr.at[i], send_sem=ysend.at[i], recv_sem=yrecv.at[i],
            device_id={"cfg": 1 - c}, device_id_type=MESH,
        )

    def stat_copy(step):
        return pltpu.make_async_remote_copy(
            src_ref=st, dst_ref=sg.at[me], send_sem=ssend.at[step - 1],
            recv_sem=srecv.at[step - 1],
            device_id={"seq": lax.rem(me + step, n)}, device_id_type=MESH,
        )

    load.wait()

    def project(j):
        weight_copy(j).wait()
        return jnp.dot(ab[...], wb[j], preferred_element_type=jnp.float32)

    def given(i, _):
        sb[i] = project(i).astype(jnp.bfloat16)
        x_copy(i).start()
        return 0

    def kept(i, _):
        own[i] = project(steps + i)
        return 0

    lax.fori_loop(0, steps, given, 0)
    lax.fori_loop(0, steps, kept, 0)

    def across(i, _):
        x_copy(i).wait()
        yb[i] = (own[i] + rb[i].astype(jnp.float32)).astype(jnp.bfloat16)
        y_copy(i).start()
        return 0

    lax.fori_loop(0, PIECES, across, 0)

    limit = counts[0:1, 0:1]
    valid = lax.broadcasted_iota(jnp.int32, (rows, part), 0) < limit
    first = jnp.full((rows, part), c, jnp.int32) == 0
    st[...] = jnp.zeros_like(st)
    for i in range(PIECES):
        span = pl.ds(i * part, part)
        x_copy(PIECES + i).wait()
        mine = (own[PIECES + i] + rb[PIECES + i].astype(jnp.float32)).astype(jnp.bfloat16)
        mine = mine.astype(jnp.float32)
        y_copy(i).wait()
        other = yr[i].astype(jnp.float32)
        conditional = jnp.where(first, mine, other)
        unconditional = jnp.where(first, other, mine)
        guided = unconditional + GUIDANCE * (conditional - unconditional)
        gb[:, span] = guided
        guided = jnp.where(valid, guided, 0.0)
        conditional = jnp.where(valid, conditional, 0.0)
        for row, field in enumerate(
            (guided, guided * guided, conditional, conditional * conditional)
        ):
            st[row:row + 1, span] = jnp.sum(field, axis=0, keepdims=True)
        st[4:5, span] = jnp.broadcast_to(limit.astype(jnp.float32), (1, part))

    for step in range(1, n):
        stat_copy(step).start()
    sg[me] = st[...]
    for step in range(1, n):
        stat_copy(step).wait()
    sums = sg[0]
    for source in range(1, n):
        sums = sums + sg[source]
    valid_total = sums[4:5, :]
    guided_mean = sums[0:1, :] / valid_total
    guided_var = sums[1:2, :] / valid_total - guided_mean * guided_mean
    cond_mean = sums[2:3, :] / valid_total
    cond_var = sums[3:4, :] / valid_total - cond_mean * cond_mean
    std_ratio = jnp.sqrt((cond_var + 1.0) / (guided_var + 1.0))
    factor = RESCALE * std_ratio + (1.0 - RESCALE)
    out[...] = (guided_mean + (gb[...] - guided_mean) * factor).astype(jnp.bfloat16)


def fused_tail(attended, out_weight, frame_counts, n):
    rows, depth = attended.shape
    width = out_weight.shape[1] // 4
    part = width // PIECES
    steps = 2 * PIECES
    bf16 = jnp.bfloat16
    f32 = jnp.float32
    counts = jnp.broadcast_to(frame_counts.reshape(1, 1), (8, HEAD_DIM))
    hbm = pl.BlockSpec(memory_space=pl.ANY)
    vmem = pl.BlockSpec(memory_space=pltpu.VMEM)
    dma = pltpu.SemaphoreType.DMA
    return pl.pallas_call(
        functools.partial(tail_kernel, n, rows, part),
        out_shape=jax.ShapeDtypeStruct((rows, width), bf16),
        in_specs=[hbm, hbm, vmem],
        out_specs=vmem,
        scratch_shapes=[
            pltpu.VMEM((rows, depth), bf16),
            pltpu.VMEM((2 * steps, depth, part), bf16),
            pltpu.VMEM((steps, rows, part), bf16),
            pltpu.VMEM((steps, rows, part), bf16),
            pltpu.VMEM((steps, rows, part), f32),
            pltpu.VMEM((PIECES, rows, part), bf16),
            pltpu.VMEM((PIECES, rows, part), bf16),
            pltpu.VMEM((rows, width), f32),
            pltpu.VMEM((8, width), f32),
            pltpu.VMEM((n, 8, width), f32),
            dma,
            dma((2 * steps,)),
            dma((steps,)),
            dma((steps,)),
            dma((PIECES,)),
            dma((PIECES,)),
            dma((n - 1,)),
            dma((n - 1,)),
        ],
        compiler_params=pltpu.CompilerParams(
            collective_id=1, has_side_effects=True, vmem_limit_bytes=62 * 1024 * 1024
        ),
    )(attended, out_weight, counts)


def body(n, cfgs, tps, queries, keys, values, text_keys, text_values, prompt_lengths, frame_counts, out_weight):
    rows, head_cols = queries.shape[1:]
    split = n % CORES == 0 and (head_cols // HEAD_DIM) % (n // CORES) == 0
    attend = attention if split and frame_counts.shape[0] == 1 else gathered_attention
    attended = attend(
        queries[0], keys[0], values[0], text_keys[0], text_values[0],
        prompt_lengths, frame_counts, n,
    )
    whole = out_weight.shape[1] % (4 * PIECES * HEAD_DIM) == 0
    if cfgs == 2 and tps == 2 and whole and frame_counts.shape[0] == 1:
        return fused_tail(attended, out_weight, frame_counts, n)
    branch = lax.psum_scatter(
        lax.dot_general(
            out_weight, attended, (((0,), (1,)), ((), ())), preferred_element_type=jnp.float32
        ).astype(jnp.bfloat16),
        "tp",
        scatter_dimension=0,
        tiled=True,
    )
    half = branch.shape[0] // cfgs
    mine = lax.axis_index("cfg")
    kept = lax.dynamic_slice_in_dim(branch, mine * half, half, 0)
    given = lax.dynamic_slice_in_dim(branch, (1 - mine) * half, half, 0)
    other = lax.ppermute(given, "cfg", [(0, 1), (1, 0)])
    first = mine == 0
    conditional = jnp.where(first, kept, other).astype(jnp.float32)
    unconditional = jnp.where(first, other, kept).astype(jnp.float32)
    guided = unconditional + GUIDANCE * (conditional - unconditional)
    valid = (jnp.arange(rows, dtype=jnp.int32) < frame_counts[0])[None, :]

    def local_sum(field):
        return jnp.sum(jnp.where(valid, field, 0.0), axis=1)

    sums = lax.psum(
        jnp.stack([
            local_sum(guided),
            local_sum(guided * guided),
            local_sum(conditional),
            local_sum(conditional * conditional),
            jnp.full((half,), frame_counts[0].astype(jnp.float32)),
        ]),
        "seq",
    )
    means = sums[:4] / sums[4:5]
    guided_mean = means[0]
    guided_var = means[1] - guided_mean * guided_mean
    cond_var = means[3] - means[2] * means[2]
    std_ratio = jnp.sqrt((cond_var + 1.0) / (guided_var + 1.0))
    factor = RESCALE * std_ratio + (1.0 - RESCALE)
    velocity = guided_mean[:, None] + (guided - guided_mean[:, None]) * factor[:, None]
    return velocity.astype(jnp.bfloat16).T


def solution(mesh):
    placed = (
        P("cfg", "seq", "tp"),
        P("cfg", "seq", "tp"),
        P("cfg", "seq", "tp"),
        P("cfg", None, "tp"),
        P("cfg", None, "tp"),
        P("cfg"),
        P("seq"),
        P("tp", None),
    )
    return jax.shard_map(
        functools.partial(body, mesh.shape["seq"], mesh.shape["cfg"], mesh.shape["tp"]),
        mesh=mesh, in_specs=placed, out_specs=P("seq", ("tp", "cfg")), check_vma=False,
    )
```

```python
import functools

import jax
import jax.numpy as jnp
from jax import lax
from jax.experimental import pallas as pl
from jax.experimental.pallas import tpu as pltpu
from jax.sharding import PartitionSpec as P

HEAD_DIM = 128
GUIDANCE = 5.0
RESCALE = 0.7
NEGATIVE = -1e30
LOG2E = 1.4426950408889634
CORES = 2
MESH = pl.DeviceIdType.MESH


def chunk_rows(total, limit):
    for unit in (256, 128, 16):
        for size in range(limit // unit * unit, 0, -unit):
            if total % size == 0:
                return size
    return total


def attention_kernel(
    n, chips, group, rows, text,
    q, k, v, tk, tv, counts, lengths,
    out,
    qb, kb, vb, tkb, tvb, cb, bias, tbias, ob,
    send, recv, fsend, frecv, csend, crecv, local, tlocal, osend, orecv,
):
    me = lax.axis_index("seq")
    core = lax.rem(me, CORES)
    chip = lax.div(me, CORES)
    partner = chip * CORES + (CORES - 1 - core)
    scale = LOG2E * HEAD_DIM ** (-0.5)

    def cols(owner, head):
        return pl.ds(pl.multiple_of((owner * group + head) * HEAD_DIM, HEAD_DIM), HEAD_DIM)

    def slot(index):
        return pl.ds(pl.multiple_of(index * rows, 16), rows)

    def chip_at(step):
        return lax.rem(chip + step, chips)

    def chip_back(step):
        return lax.rem(chip + chips - step, chips)

    barrier = pltpu.get_barrier_semaphore()
    for step in range(1, n):
        pl.semaphore_signal(
            barrier, inc=1, device_id={"seq": lax.rem(me + step, n)}, device_id_type=MESH
        )
    pl.semaphore_wait(barrier, n - 1)

    def count_copy(step):
        return pltpu.make_async_remote_copy(
            src_ref=counts, dst_ref=cb.at[me], send_sem=csend.at[step - 1],
            recv_sem=crecv.at[step - 1],
            device_id={"seq": lax.rem(me + step, n)}, device_id_type=MESH,
        )

    def block_copies(head, step):
        target = chip_at(step)
        device = {"seq": target * CORES + core}
        made = []
        for index, (src, dst) in enumerate(
            ((k, kb.at[head, slot(me)]), (v, vb.at[head, slot(me)]), (q, qb.at[head, chip]))
        ):
            made.append(pltpu.make_async_remote_copy(
                src_ref=src.at[:, cols(target, head)], dst_ref=dst,
                send_sem=send.at[index, head, step - 1],
                recv_sem=recv.at[index, head, step - 1],
                device_id=device, device_id_type=MESH,
            ))
        return made

    def own_copies(head):
        return [
            pltpu.make_async_copy(k.at[:, cols(chip, head)], kb.at[head, slot(me)], local.at[0, head]),
            pltpu.make_async_copy(v.at[:, cols(chip, head)], vb.at[head, slot(me)], local.at[1, head]),
            pltpu.make_async_copy(q.at[:, cols(chip, head)], qb.at[head, chip], local.at[2, head]),
            pltpu.make_async_copy(tk.at[:, cols(chip, head)], tkb.at[head], tlocal.at[0, head]),
            pltpu.make_async_copy(tv.at[:, cols(chip, head)], tvb.at[head], tlocal.at[1, head]),
        ]

    def own_forward(head):
        return [
            pltpu.make_async_remote_copy(
                src_ref=src.at[:, cols(chip, head)], dst_ref=dst.at[head, slot(me)],
                send_sem=fsend.at[index, head, 0], recv_sem=frecv.at[index, head, 0],
                device_id={"seq": partner}, device_id_type=MESH,
            )
            for index, (src, dst) in enumerate(((k, kb), (v, vb)))
        ]

    def forward(index, head, step):
        buf = (kb, vb)[index]
        where = slot(chip_back(step) * CORES + core)
        return pltpu.make_async_remote_copy(
            src_ref=buf.at[head, where], dst_ref=buf.at[head, where],
            send_sem=fsend.at[index, head, step], recv_sem=frecv.at[index, head, step],
            device_id={"seq": partner}, device_id_type=MESH,
        )

    def out_copy(head, step):
        target = chip_at(step)
        return pltpu.make_async_remote_copy(
            src_ref=ob.at[head, target], dst_ref=out.at[:, cols(chip, head)],
            send_sem=osend.at[head, step], recv_sem=orecv.at[head, step],
            device_id={"seq": target * CORES + core}, device_id_type=MESH,
        )

    def own_out(head):
        return pltpu.make_async_copy(
            ob.at[head, chip], out.at[:, cols(chip, head)], osend.at[head, 0]
        )

    for step in range(1, n):
        count_copy(step).start()

    def start_head(head, _):
        for step in range(1, chips):
            for copy in block_copies(head, step):
                copy.start()
        for copy in own_copies(head):
            copy.start()
        for copy in own_forward(head):
            copy.start()
        return 0

    lax.fori_loop(0, group, start_head, 0)

    cb[me] = counts[...]
    for step in range(1, n):
        count_copy(step).wait()
    lane = lax.broadcasted_iota(jnp.int32, (rows, HEAD_DIM), 1)
    place = lax.broadcasted_iota(jnp.int32, (rows, HEAD_DIM), 0)
    for source in range(n):
        limit = cb[source][0:1, :]
        bias[source * rows:(source + 1) * rows, :] = jnp.where(
            (lane == 0) & (place >= limit), NEGATIVE, 0.0
        ).astype(jnp.bfloat16)
    tlane = lax.broadcasted_iota(jnp.int32, (text, HEAD_DIM), 1)
    tplace = lax.broadcasted_iota(jnp.int32, (text, HEAD_DIM), 0)
    tbias[...] = jnp.where(
        (tlane == 0) & (tplace >= lengths[0:1, :]), NEGATIVE, 0.0
    ).astype(jnp.bfloat16)

    total = n * rows
    size = chunk_rows(total, 768)

    def ones(length):
        return jnp.where(
            lax.broadcasted_iota(jnp.int32, (length, HEAD_DIM), 1) == 0, 1.0, 0.0
        ).astype(jnp.bfloat16)

    def one_head(head, _):
        for copy in own_copies(head):
            copy.wait()
        for step in range(1, chips):
            made = block_copies(head, step)
            for index in range(2):
                made[index].wait()
                forward(index, head, step).start()
            made[2].wait()
        for copy in own_forward(head):
            copy.wait()
        for step in range(1, chips):
            for index in range(2):
                forward(index, head, step).wait()

        def one_block(step):
            target = chip_at(step)
            query = jnp.concatenate([qb[head, target], ones(rows)], axis=1)

            def piece(state, keys, masks, vals):
                keys = jnp.concatenate([keys, masks], axis=1)
                vals = jnp.concatenate([vals, ones(vals.shape[0])], axis=1)
                scores = lax.dot_general(
                    query, keys, (((1,), (1,)), ((), ())), preferred_element_type=jnp.float32
                )
                high = jnp.max(scores, axis=1, keepdims=True) * scale
                if state is not None:
                    high = jnp.maximum(high, state[0])
                weights = jnp.exp2(scores * scale - high).astype(jnp.bfloat16)
                mixed = jnp.dot(weights, vals, preferred_element_type=jnp.float32)
                if state is not None:
                    mixed = mixed + state[1] * jnp.exp2(state[0] - high)
                return (high, mixed)

            state = piece(None, tkb[head], tbias[...], tvb[head])
            for start in range(0, total, size):
                span = pl.ds(start, size)
                state = piece(state, kb[head, span], bias[span, :], vb[head, span])
            mixed = state[1]
            ob[head, target] = (
                mixed[:, :HEAD_DIM] / mixed[:, HEAD_DIM:HEAD_DIM + 1]
            ).astype(jnp.bfloat16)

        def far_block(step, _):
            one_block(step)
            out_copy(head, step).start()
            return 0

        lax.fori_loop(1, chips, far_block, 0)
        one_block(0)
        own_out(head).start()
        return 0

    lax.fori_loop(0, group, one_head, 0)

    def finish(head, _):
        for step in range(1, chips):
            out_copy(head, step).wait()
        own_out(head).wait()
        return 0

    lax.fori_loop(0, group, finish, 0)


def attention(queries, keys, values, text_keys, text_values, prompt_lengths, frame_counts, n):
    rows, width = queries.shape
    text = text_keys.shape[0]
    chips = n // CORES
    heads = width // HEAD_DIM
    group = heads // chips
    counts = jnp.broadcast_to(frame_counts.reshape(1, 1), (8, HEAD_DIM))
    lengths = jnp.broadcast_to(prompt_lengths.reshape(1, 1), (8, HEAD_DIM))
    bf16 = jnp.bfloat16
    total = n * rows
    hbm = pl.BlockSpec(memory_space=pl.ANY)
    vmem = pl.BlockSpec(memory_space=pltpu.VMEM)
    dma = pltpu.SemaphoreType.DMA
    return pl.pallas_call(
        functools.partial(attention_kernel, n, chips, group, rows, text),
        out_shape=jax.ShapeDtypeStruct((rows, width), bf16),
        in_specs=[hbm] * 5 + [vmem] * 2,
        out_specs=hbm,
        scratch_shapes=[
            pltpu.VMEM((group, chips, rows, HEAD_DIM), bf16),
            pltpu.VMEM((group, total, HEAD_DIM), bf16),
            pltpu.VMEM((group, total, HEAD_DIM), bf16),
            pltpu.VMEM((group, text, HEAD_DIM), bf16),
            pltpu.VMEM((group, text, HEAD_DIM), bf16),
            pltpu.VMEM((n, 8, HEAD_DIM), jnp.int32),
            pltpu.VMEM((total, HEAD_DIM), bf16),
            pltpu.VMEM((text, HEAD_DIM), bf16),
            pltpu.VMEM((group, chips, rows, HEAD_DIM), bf16),
            dma((3, group, chips - 1)),
            dma((3, group, chips - 1)),
            dma((2, group, chips)),
            dma((2, group, chips)),
            dma((n - 1,)),
            dma((n - 1,)),
            dma((3, group)),
            dma((2, group)),
            dma((group, chips)),
            dma((group, chips)),
        ],
        compiler_params=pltpu.CompilerParams(
            collective_id=0, has_side_effects=True, vmem_limit_bytes=62 * 1024 * 1024
        ),
    )(queries, keys, values, text_keys, text_values, counts, lengths)


def frame_valid(positions, counts_table, slots):
    frame_index = positions // slots
    slot_index = positions % slots
    frame_ids = jnp.arange(counts_table.shape[0], dtype=jnp.int32)
    frame_limit = jnp.sum(
        jnp.where(frame_index[:, None] == frame_ids[None, :], counts_table[None, :], 0), axis=1
    )
    return slot_index < frame_limit


def attend_block(carry, key_rows, value_rows, query_heads, key_mask):
    row_max, weight_sum, mixed_sum = carry
    head_count = query_heads.shape[1]
    key_heads = key_rows.reshape(key_rows.shape[0], head_count, HEAD_DIM)
    value_heads = value_rows.reshape(value_rows.shape[0], head_count, HEAD_DIM)
    scores = jnp.einsum(
        "qhd,khd->hqk", query_heads, key_heads, preferred_element_type=jnp.float32
    ) * HEAD_DIM ** (-0.5)
    scores = jnp.where(key_mask[None, None, :], scores, NEGATIVE)
    new_max = jnp.maximum(row_max, jnp.max(scores, axis=2))
    shrink = jnp.exp(row_max - new_max)
    weights = jnp.exp(scores - new_max[:, :, None])
    weight_sum = weight_sum * shrink + jnp.sum(weights, axis=2)
    mixed_sum = mixed_sum * shrink[:, :, None] + jnp.einsum(
        "hqk,khd->hqd",
        weights.astype(jnp.bfloat16),
        value_heads,
        preferred_element_type=jnp.float32,
    )
    return (new_max, weight_sum, mixed_sum)


def gathered_attention(
    queries, keys, values, text_keys, text_values, prompt_lengths, frame_counts, n
):
    row_count, head_cols = queries.shape
    head_count = head_cols // HEAD_DIM
    all_counts = lax.all_gather(frame_counts, "seq", axis=0, tiled=True)
    query_heads = queries.reshape(row_count, head_count, HEAD_DIM)
    text_mask = jnp.arange(text_keys.shape[0], dtype=jnp.int32) < prompt_lengths[0]
    empty_state = (
        jnp.full((head_count, row_count), NEGATIVE, jnp.float32),
        jnp.zeros((head_count, row_count), jnp.float32),
        jnp.zeros((head_count, row_count, HEAD_DIM), jnp.float32),
    )
    text_state = attend_block(empty_state, text_keys, text_values, query_heads, text_mask)
    key_rows = lax.all_gather(keys, "seq", axis=0, tiled=True)
    value_rows = lax.all_gather(values, "seq", axis=0, tiled=True)
    positions = jnp.arange(key_rows.shape[0], dtype=jnp.int32)
    _, weight_sum, mixed_sum = attend_block(
        text_state, key_rows, value_rows, query_heads,
        frame_valid(positions, all_counts, row_count // frame_counts.shape[0]),
    )
    return (
        jnp.transpose(mixed_sum / weight_sum[:, :, None], (1, 0, 2))
        .reshape(row_count, head_cols)
        .astype(jnp.bfloat16)
    )


PIECES = 5


def tail_kernel(
    n, rows, part,
    att, w, counts,
    out,
    ab, wb, sb, rb, own, yb, yr, gb, st, sg,
    asem, wsem, xsend, xrecv, ysend, yrecv, ssend, srecv,
):
    me = lax.axis_index("seq")
    t = lax.axis_index("tp")
    c = lax.axis_index("cfg")
    steps = 2 * PIECES
    width = PIECES * part

    def column(side, index):
        far = lax.div(index, PIECES)
        branch = far * c + (1 - far) * (1 - c)
        return (side * 2 + branch) * width + lax.rem(index, PIECES) * part

    def weight_copy(j):
        far = lax.div(j, steps)
        side = far * t + (1 - far) * (1 - t)
        start = pl.multiple_of(column(side, lax.rem(j, steps)), HEAD_DIM)
        return pltpu.make_async_copy(w.at[:, pl.ds(start, part)], wb.at[j], wsem.at[j])

    load = pltpu.make_async_copy(att, ab, asem)
    load.start()

    def start_weight(j, _):
        weight_copy(j).start()
        return 0

    lax.fori_loop(0, 2 * steps, start_weight, 0)

    barrier = pltpu.get_barrier_semaphore()
    pl.semaphore_signal(barrier, inc=1, device_id={"tp": 1 - t}, device_id_type=MESH)
    pl.semaphore_signal(barrier, inc=1, device_id={"cfg": 1 - c}, device_id_type=MESH)
    for step in range(1, n):
        pl.semaphore_signal(
            barrier, inc=1, device_id={"seq": lax.rem(me + step, n)}, device_id_type=MESH
        )
    pl.semaphore_wait(barrier, n + 1)

    def x_copy(i):
        return pltpu.make_async_remote_copy(
            src_ref=sb.at[i], dst_ref=rb.at[i], send_sem=xsend.at[i], recv_sem=xrecv.at[i],
            device_id={"tp": 1 - t}, device_id_type=MESH,
        )

    def y_copy(i):
        return pltpu.make_async_remote_copy(
            src_ref=yb.at[i], dst_ref=yr.at[i], send_sem=ysend.at[i], recv_sem=yrecv.at[i],
            device_id={"cfg": 1 - c}, device_id_type=MESH,
        )

    def stat_copy(step):
        return pltpu.make_async_remote_copy(
            src_ref=st, dst_ref=sg.at[me], send_sem=ssend.at[step - 1],
            recv_sem=srecv.at[step - 1],
            device_id={"seq": lax.rem(me + step, n)}, device_id_type=MESH,
        )

    load.wait()

    def project(j):
        weight_copy(j).wait()
        return jnp.dot(ab[...], wb[j], preferred_element_type=jnp.float32)

    def given(i, _):
        sb[i] = project(i).astype(jnp.bfloat16)
        x_copy(i).start()
        return 0

    def kept(i, _):
        own[i] = project(steps + i)
        return 0

    lax.fori_loop(0, steps, given, 0)
    lax.fori_loop(0, steps, kept, 0)

    def across(i, _):
        x_copy(i).wait()
        yb[i] = (own[i] + rb[i].astype(jnp.float32)).astype(jnp.bfloat16)
        y_copy(i).start()
        return 0

    lax.fori_loop(0, PIECES, across, 0)

    limit = counts[0:1, 0:1]
    valid = lax.broadcasted_iota(jnp.int32, (rows, part), 0) < limit
    first = jnp.full((rows, part), c, jnp.int32) == 0
    st[...] = jnp.zeros_like(st)
    for i in range(PIECES):
        span = pl.ds(i * part, part)
        x_copy(PIECES + i).wait()
        mine = (own[PIECES + i] + rb[PIECES + i].astype(jnp.float32)).astype(jnp.bfloat16)
        mine = mine.astype(jnp.float32)
        y_copy(i).wait()
        other = yr[i].astype(jnp.float32)
        conditional = jnp.where(first, mine, other)
        unconditional = jnp.where(first, other, mine)
        guided = unconditional + GUIDANCE * (conditional - unconditional)
        gb[:, span] = guided
        guided = jnp.where(valid, guided, 0.0)
        conditional = jnp.where(valid, conditional, 0.0)
        for row, field in enumerate(
            (guided, guided * guided, conditional, conditional * conditional)
        ):
            st[row:row + 1, span] = jnp.sum(field, axis=0, keepdims=True)
        st[4:5, span] = jnp.broadcast_to(limit.astype(jnp.float32), (1, part))

    for step in range(1, n):
        stat_copy(step).start()
    sg[me] = st[...]
    for step in range(1, n):
        stat_copy(step).wait()
    sums = sg[0]
    for source in range(1, n):
        sums = sums + sg[source]
    valid_total = sums[4:5, :]
    guided_mean = sums[0:1, :] / valid_total
    guided_var = sums[1:2, :] / valid_total - guided_mean * guided_mean
    cond_mean = sums[2:3, :] / valid_total
    cond_var = sums[3:4, :] / valid_total - cond_mean * cond_mean
    std_ratio = jnp.sqrt((cond_var + 1.0) / (guided_var + 1.0))
    factor = RESCALE * std_ratio + (1.0 - RESCALE)
    out[...] = (guided_mean + (gb[...] - guided_mean) * factor).astype(jnp.bfloat16)


def fused_tail(attended, out_weight, frame_counts, n):
    rows, depth = attended.shape
    width = out_weight.shape[1] // 4
    part = width // PIECES
    steps = 2 * PIECES
    bf16 = jnp.bfloat16
    f32 = jnp.float32
    counts = jnp.broadcast_to(frame_counts.reshape(1, 1), (8, HEAD_DIM))
    hbm = pl.BlockSpec(memory_space=pl.ANY)
    vmem = pl.BlockSpec(memory_space=pltpu.VMEM)
    dma = pltpu.SemaphoreType.DMA
    return pl.pallas_call(
        functools.partial(tail_kernel, n, rows, part),
        out_shape=jax.ShapeDtypeStruct((rows, width), bf16),
        in_specs=[hbm, hbm, vmem],
        out_specs=vmem,
        scratch_shapes=[
            pltpu.VMEM((rows, depth), bf16),
            pltpu.VMEM((2 * steps, depth, part), bf16),
            pltpu.VMEM((steps, rows, part), bf16),
            pltpu.VMEM((steps, rows, part), bf16),
            pltpu.VMEM((steps, rows, part), f32),
            pltpu.VMEM((PIECES, rows, part), bf16),
            pltpu.VMEM((PIECES, rows, part), bf16),
            pltpu.VMEM((rows, width), f32),
            pltpu.VMEM((8, width), f32),
            pltpu.VMEM((n, 8, width), f32),
            dma,
            dma((2 * steps,)),
            dma((steps,)),
            dma((steps,)),
            dma((PIECES,)),
            dma((PIECES,)),
            dma((n - 1,)),
            dma((n - 1,)),
        ],
        compiler_params=pltpu.CompilerParams(
            collective_id=1, has_side_effects=True, vmem_limit_bytes=62 * 1024 * 1024
        ),
    )(attended, out_weight, counts)


def body(n, cfgs, tps, queries, keys, values, text_keys, text_values, prompt_lengths, frame_counts, out_weight):
    rows, head_cols = queries.shape[1:]
    split = n % CORES == 0 and (head_cols // HEAD_DIM) % (n // CORES) == 0
    attend = attention if split and frame_counts.shape[0] == 1 else gathered_attention
    attended = attend(
        queries[0], keys[0], values[0], text_keys[0], text_values[0],
        prompt_lengths, frame_counts, n,
    )
    whole = out_weight.shape[1] % (4 * PIECES * HEAD_DIM) == 0
    if cfgs == 2 and tps == 2 and whole and frame_counts.shape[0] == 1:
        return fused_tail(attended, out_weight, frame_counts, n)
    branch = lax.psum_scatter(
        lax.dot_general(
            out_weight, attended, (((0,), (1,)), ((), ())), preferred_element_type=jnp.float32
        ).astype(jnp.bfloat16),
        "tp",
        scatter_dimension=0,
        tiled=True,
    )
    half = branch.shape[0] // cfgs
    mine = lax.axis_index("cfg")
    kept = lax.dynamic_slice_in_dim(branch, mine * half, half, 0)
    given = lax.dynamic_slice_in_dim(branch, (1 - mine) * half, half, 0)
    other = lax.ppermute(given, "cfg", [(0, 1), (1, 0)])
    first = mine == 0
    conditional = jnp.where(first, kept, other).astype(jnp.float32)
    unconditional = jnp.where(first, other, kept).astype(jnp.float32)
    guided = unconditional + GUIDANCE * (conditional - unconditional)
    valid = (jnp.arange(rows, dtype=jnp.int32) < frame_counts[0])[None, :]

    def local_sum(field):
        return jnp.sum(jnp.where(valid, field, 0.0), axis=1)

    sums = lax.psum(
        jnp.stack([
            local_sum(guided),
            local_sum(guided * guided),
            local_sum(conditional),
            local_sum(conditional * conditional),
            jnp.full((half,), frame_counts[0].astype(jnp.float32)),
        ]),
        "seq",
    )
    means = sums[:4] / sums[4:5]
    guided_mean = means[0]
    guided_var = means[1] - guided_mean * guided_mean
    cond_var = means[3] - means[2] * means[2]
    std_ratio = jnp.sqrt((cond_var + 1.0) / (guided_var + 1.0))
    factor = RESCALE * std_ratio + (1.0 - RESCALE)
    velocity = guided_mean[:, None] + (guided - guided_mean[:, None]) * factor[:, None]
    return velocity.astype(jnp.bfloat16).T


def solution(mesh):
    placed = (
        P("cfg", "seq", "tp"),
        P("cfg", "seq", "tp"),
        P("cfg", "seq", "tp"),
        P("cfg", None, "tp"),
        P("cfg", None, "tp"),
        P("cfg"),
        P("seq"),
        P("tp", None),
    )
    return jax.shard_map(
        functools.partial(body, mesh.shape["seq"], mesh.shape["cfg"], mesh.shape["tp"]),
        mesh=mesh, in_specs=placed, out_specs=P("seq", ("tp", "cfg")), check_vma=False,
    )
```
